32 devices in a mesh: dp: 16 (over z, y, core), tensor: 2 (over x).
Axes of the slice: x: 2, y: 2, z: 4, core: 2. Of those that a mesh axis runs over, the one named last changes fastest.
Arguments:
- training_token_input: bfloat16 [4096, 8192], P('dp', 'tensor'), may hold values from -6 to 6
- gate_output_gradient: bfloat16 [4096, 29568], P('dp', 'tensor'), may hold values from -6 to 6
- up_output_gradient: bfloat16 [4096, 29568], P('dp', 'tensor'), may hold values from -6 to 6
- gate_first_matrix: bfloat16 [8192, 64], P('tensor'), may hold values from -0.0625 to 0.0625
- gate_second_matrix: bfloat16 [64, 29568], P(None, 'tensor'), may hold values from -0.75 to 0.75
- up_first_matrix: bfloat16 [8192, 64], P('tensor'), may hold values from -0.0625 to 0.0625
- up_second_matrix: bfloat16 [64, 29568], P(None, 'tensor'), may hold values from -0.75 to 0.75
- gate_weight_base: bfloat16 [8192, 29568], P('tensor', 'dp'), may hold values from -0.0625 to 0.0625
- up_weight_base: bfloat16 [8192, 29568], P('tensor', 'dp'), may hold values from -0.0625 to 0.0625
- down_weight_base: bfloat16 [29568, 8192], P('dp', 'tensor'), may hold values from -0.03125 to 0.03125
- decode_step_input: bfloat16 [2, 512, 8192], P(None, None, 'tensor'), may hold values from -6 to 6
Outputs:
- decoded: bfloat16 [2, 512, 8192], P(None, None, 'tensor')
The draws below stay inside these ranges and needn't reach their ends.
All inputs are finite; a program needn't handle non-finite values.
Results may differ from the reference program's by a relative error of at most 0.04.
Values may be sent and summed in bfloat16 or wider, within the bound.
A program may use at most 192 MiB of HBM per device.

```python
import math
import jax
import jax.numpy as jnp
from jax import lax

MODEL_WIDTH = 8192
HIDDEN_UNITS = 29568
ADAPTER_RANK = 64
ROWS = 512
STEPS = 2
TOKENS = 4096
N_TENSOR = 2


def levels(own_key, shape, split, low, high):
    def one(dim, blocks):
        draws = jax.random.uniform(jax.random.fold_in(jax.random.fold_in(own_key, 6), dim), (blocks,), jnp.float32, low / len(split), high / len(split))
        return jnp.repeat(jnp.exp(draws), shape[dim] // blocks).reshape((-1,) + (1,) * (len(shape) - dim - 1))

    level = one(*split[0])
    for cut in split[1:]:
        level = level * one(*cut)
    return level


def centred(own_key, dims, scale, bound, cuts=(), kind=jnp.bfloat16):
    entries = jax.random.normal(own_key, dims, jnp.float32) * scale
    if len(cuts) > 0:
        entries = levels(own_key, dims, cuts, -0.22, 0.18) * entries
    return jnp.clip(entries, min=-bound, max=bound).astype(kind)


def setup_inputs(seed: int = 0) -> dict:
    splits = jax.random.split(jax.random.key(seed), 12)
    training_token_input = centred(splits[0], (TOKENS, MODEL_WIDTH), 1.0, 6.0, ((0, 16), (1, 2)))
    gate_output_gradient = centred(splits[1], (TOKENS, HIDDEN_UNITS), 1.0, 6.0, ((0, 16), (1, 2)))
    up_output_gradient = centred(splits[2], (TOKENS, HIDDEN_UNITS), 1.0, 6.0, ((0, 16), (1, 2)))
    gate_first_matrix = centred(splits[3], (MODEL_WIDTH, ADAPTER_RANK), MODEL_WIDTH ** -0.5, 0.0625, ((0, 2),))
    gate_second_matrix = centred(splits[4], (ADAPTER_RANK, HIDDEN_UNITS), ADAPTER_RANK ** -0.5, 0.75, ((1, 2),))
    up_first_matrix = centred(splits[5], (MODEL_WIDTH, ADAPTER_RANK), MODEL_WIDTH ** -0.5, 0.0625, ((0, 2),))
    up_second_matrix = centred(splits[6], (ADAPTER_RANK, HIDDEN_UNITS), ADAPTER_RANK ** -0.5, 0.75, ((1, 2),))
    gate_weight_base = centred(splits[7], (MODEL_WIDTH, HIDDEN_UNITS), MODEL_WIDTH ** -0.5, 0.0625, ((0, 2), (1, 16)))
    up_weight_base = centred(splits[8], (MODEL_WIDTH, HIDDEN_UNITS), MODEL_WIDTH ** -0.5, 0.0625, ((0, 2), (1, 16)))
    down_weight_base = centred(splits[9], (HIDDEN_UNITS, MODEL_WIDTH), HIDDEN_UNITS ** -0.5, 0.03125, ((0, 16), (1, 2)))
    decode_step_input = centred(splits[10], (STEPS, ROWS, MODEL_WIDTH), 1.0, 6.0, ((2, 2),))
    return {"training_token_input": training_token_input, "gate_output_gradient": gate_output_gradient, "up_output_gradient": up_output_gradient, "gate_first_matrix": gate_first_matrix, "gate_second_matrix": gate_second_matrix, "up_first_matrix": up_first_matrix, "up_second_matrix": up_second_matrix, "gate_weight_base": gate_weight_base, "up_weight_base": up_weight_base, "down_weight_base": down_weight_base, "decode_step_input": decode_step_input}


def partial_rounded(inputs, weight):
    blocks = jnp.moveaxis(inputs.reshape(inputs.shape[0], N_TENSOR, -1), 1, 0)
    pieces = weight.reshape(N_TENSOR, -1, weight.shape[1])

    def one_block(pair):
        left, right = pair
        total = jnp.dot(left, right, preferred_element_type=jnp.float32)
        return lax.optimization_barrier(total.astype(jnp.bfloat16)).astype(jnp.float32)
    terms = lax.map(one_block, (blocks, pieces))
    return lax.optimization_barrier(jnp.sum(terms, axis=0))

def reference(training_token_input, gate_output_gradient, up_output_gradient, gate_first_matrix, gate_second_matrix, up_first_matrix, up_second_matrix, gate_weight_base, up_weight_base, down_weight_base, decode_step_input):
    second_learning_rate = 0.5 / math.sqrt(ADAPTER_RANK * TOKENS)
    first_learning_rate = 0.5 / math.sqrt(MODEL_WIDTH * HIDDEN_UNITS * TOKENS / ADAPTER_RANK)

    def apply_adapter(cotangent, factor_b, factor_a, base):
        inner_b = jnp.dot(training_token_input, factor_b, preferred_element_type=jnp.float32).astype(jnp.bfloat16)
        inner_a = jnp.dot(cotangent, factor_a.T, preferred_element_type=jnp.float32).astype(jnp.bfloat16)
        grad_a = jnp.dot(inner_b.T, cotangent, preferred_element_type=jnp.float32)
        grad_b = jnp.dot(training_token_input.T, inner_a, preferred_element_type=jnp.float32)
        fresh_b = (factor_b.astype(jnp.float32) - first_learning_rate * grad_b).astype(jnp.bfloat16)
        fresh_a = (factor_a.astype(jnp.float32) - second_learning_rate * grad_a).astype(jnp.bfloat16)
        update = jnp.dot(fresh_b, fresh_a, preferred_element_type=jnp.float32)
        return (base.astype(jnp.float32) + update).astype(jnp.bfloat16)
    combined_gate_weight = apply_adapter(gate_output_gradient, gate_first_matrix, gate_second_matrix, gate_weight_base)
    combined_up_weight = apply_adapter(up_output_gradient, up_first_matrix, up_second_matrix, up_weight_base)
    results = []
    for position in range(STEPS):
        rows_in = decode_step_input[position]
        gate = partial_rounded(rows_in, combined_gate_weight)
        upper = partial_rounded(rows_in, combined_up_weight)
        hidden = (jax.nn.silu(gate) * upper).astype(jnp.bfloat16)
        results.append(jnp.dot(hidden, down_weight_base, preferred_element_type=jnp.float32).astype(jnp.bfloat16))
    return jnp.stack(results)
```

```python
import functools
import math

import jax
import jax.numpy as jnp
from jax import lax
from jax.experimental import pallas as pl
from jax.experimental.pallas import tpu as pltpu
from jax.sharding import PartitionSpec as P

MODEL_WIDTH = 8192
HIDDEN_UNITS = 29568
ADAPTER_RANK = 64
MESH = pl.DeviceIdType.MESH
F32, BF16 = jnp.float32, jnp.bfloat16


def swap(value):
    return lax.ppermute(value, "tensor", ((0, 1), (1, 0)))


def pair_sum(value):
    if lax.axis_size("tensor") == 2:
        sent = value.astype(jnp.bfloat16)
        return sent.astype(jnp.float32) + swap(sent).astype(jnp.float32)
    return lax.psum(value.astype(jnp.bfloat16), "tensor").astype(jnp.float32)


def row_share(value, index):
    rows = value.shape[1] // lax.axis_size("tensor")
    return lax.dynamic_slice_in_dim(value, index * rows, rows, 1)


class Place:
    def __init__(self, n_dp):
        self.chips = n_dp // 2
        depth = self.chips // 2
        dp = lax.axis_index("dp")
        self.t = lax.axis_index("tensor")
        self.core = lax.rem(dp, 2)
        y = lax.rem(dp // 2, 2)
        z = dp // 4
        where = jnp.where(y == 0, z, self.chips - 1 - z)
        self.turn = jnp.where(self.core == 0, where, lax.rem(self.chips - where, self.chips))

        def chip(position):
            position = lax.rem(position + self.chips, self.chips)
            up = position < depth
            there = jnp.where(up, position * 2, (self.chips - 1 - position) * 2 + 1)
            return (there * 2 + self.core, self.t)

        step = jnp.where(self.core == 0, 1, -1)
        self.after = chip(where + step)
        self.before = chip(where - step)
        self.across = (dp, 1 - self.t)
        self.mate = (dp + 1 - 2 * self.core, self.t)


def remote(src, dst, send, recv, target):
    return pltpu.make_async_remote_copy(
        src_ref=src, dst_ref=dst, send_sem=send, recv_sem=recv, device_id=target, device_id_type=MESH
    )


def greet(targets):
    barrier = pltpu.get_barrier_semaphore()
    for target in targets:
        pl.semaphore_signal(barrier, inc=1, device_id=target, device_id_type=MESH)
    pl.semaphore_wait(barrier, len(targets))


def tail_kernel(
    n_dp, chunks, steps, hidden_ref, down_ref, out_ref,
    weight, rows, keep, give, take, ring, result,
    weight_sem, load_sem, store_sem, across_send, across_recv, mate_send, mate_recv,
    sum_send, sum_recv, all_send, all_recv, copy_send, copy_recv,
):
    place = Place(n_dp)
    n = place.chips
    half = weight.shape[1] // 2
    part = rows.shape[1] // 2
    shard = 2 * part // n
    tile = min(512, half)
    tiles = half // tile
    mine = pl.multiple_of(place.core * half, half)
    other = pl.multiple_of((1 - place.core) * half, half)

    weight_parts = 4
    width = weight.shape[1] // weight_parts

    def weight_copy(i):
        block = pl.ds(i * width, width)
        return pltpu.make_async_copy(down_ref.at[:, block], weight.at[:, block], weight_sem.at[i])

    def own_rows(q):
        return rows.at[q, pl.ds(pl.multiple_of(place.t * part, part), part), :]

    loads = [
        pltpu.make_async_copy(hidden_ref.at[pl.ds(q * part, part), :], own_rows(q), load_sem.at[q])
        for q in range(chunks)
    ]
    for load in loads:
        load.start()
    for i in range(weight_parts):
        weight_copy(i).start()
    greet((place.across, place.mate, place.after, place.before))
    crossing = []
    for q in range(chunks):
        loads[q].wait()
        copy = remote(own_rows(q), own_rows(q), across_send.at[q], across_recv.at[q], place.across)
        copy.start()
        crossing.append(copy)
    for i in range(weight_parts):
        weight_copy(i).wait()

    pending = []

    def shard_rows(index):
        index = lax.rem(index + 2 * n, n)
        return pl.ds(pl.multiple_of(index * shard, shard), shard)

    def product(q, i, target, start):
        block = pl.ds(pl.multiple_of(start + i * tile, tile), tile)
        value = jnp.dot(rows[q], weight[:, block], preferred_element_type=F32)
        target[q, :, pl.ds(i * tile, tile)] = value.astype(BF16)

    def stages(q):
        crossing[q].wait_recv()
        for i in range(tiles):
            product(q, i, give, other)
            if i == tiles - 1:
                exchange = remote(give.at[q], take.at[q], mate_send.at[q], mate_recv.at[q], place.mate)
                exchange.start()
            yield "product"
        for i in range(tiles):
            product(q, i, keep, mine)
            yield "product"
        exchange.wait()
        yield "product"

        def total(index):
            own = shard_rows(index)
            return keep[q, own, :].astype(F32) + take[q, own, :].astype(F32)

        for s in range(n):
            own = shard_rows(place.turn - s)
            value = total(place.turn - s)
            if s > 0:
                hop.wait()
                value = value + ring[q, s - 1].astype(F32)
            if s < n - 1:
                keep[q, own, :] = value.astype(BF16)
                hop = remote(keep.at[q, own, :], ring.at[q, s], sum_send.at[q, s], sum_recv.at[q, s], place.after)
                hop.start()
            else:
                result[q, own, pl.ds(mine, half)] = value.astype(BF16)
            if s < n - 1:
                yield "ring"
        copies = []
        for s in range(n):
            block = result.at[q, shard_rows(place.turn + 1 - s), pl.ds(mine, half)]
            if s > 0:
                hop.wait()
            if s < n - 1:
                hop = remote(block, block, all_send.at[q, s], all_recv.at[q, s], place.after)
                hop.start()
            copy = remote(block, block, copy_send.at[q, s], copy_recv.at[q, s], place.mate)
            copy.start()
            copies.append(copy)
            yield "ring"
        for copy in copies:
            copy.wait()
        count = 2 * part * chunks // steps
        per = chunks // steps
        for side in range(2):
            first = (q // per) * count + side * (count // 2) + (q % per) * part
            store = pltpu.make_async_copy(
                result.at[q, pl.ds(side * part, part), :], out_ref.at[pl.ds(first, part), :], store_sem.at[q, side]
            )
            store.start()
            pending.append(store)

    live = [stages(q) for q in range(chunks)]
    active, waiting = [], list(range(chunks))
    first = waiting.pop(0)
    while next(live[first]) == "product":
        pass
    active.append(first)
    building = waiting.pop(0) if waiting else None
    while active or building is not None:
        if building is not None:
            for _ in range(2):
                if building is not None and next(live[building]) == "ring":
                    active.append(building)
                    building = waiting.pop(0) if waiting else None
                    break
        for q in list(active):
            if next(live[q], None) is None:
                active.remove(q)
    for store in pending:
        store.wait()
    for copy in crossing:
        copy.wait_send()


def tail(hidden, down, steps):
    n_dp = lax.axis_size("dp")
    n = n_dp // 2
    count, units = hidden.shape
    width = down.shape[1]
    chunks = 4
    part = count // chunks
    both = 2 * part
    dma = pltpu.SemaphoreType.DMA
    anywhere = pl.BlockSpec(memory_space=pl.ANY)
    return pl.pallas_call(
        functools.partial(tail_kernel, n_dp, chunks, steps),
        out_shape=jax.ShapeDtypeStruct((2 * count, width), BF16),
        in_specs=[anywhere, anywhere],
        out_specs=anywhere,
        scratch_shapes=[
            pltpu.VMEM((units, width), BF16),
            pltpu.VMEM((chunks, both, units), BF16),
            pltpu.VMEM((chunks, both, width // 2), BF16),
            pltpu.VMEM((chunks, both, width // 2), BF16),
            pltpu.VMEM((chunks, both, width // 2), BF16),
            pltpu.VMEM((chunks, n - 1, both // n, width // 2), BF16),
            pltpu.VMEM((chunks, both, width), BF16),
            dma((4,)), dma((chunks,)), dma((chunks, 2)),
            dma((chunks,)), dma((chunks,)), dma((chunks,)), dma((chunks,)),
            dma((chunks, n)), dma((chunks, n)), dma((chunks, n)), dma((chunks, n)),
            dma((chunks, n)), dma((chunks, n)),
        ],
        compiler_params=pltpu.CompilerParams(
            collective_id=0, has_side_effects=True, vmem_limit_bytes=60 * 1024 * 1024
        ),
        name="tail",
    )(hidden, down)


def shift_dp(value, move):
    n_dp = lax.axis_size("dp")
    return lax.ppermute(value, "dp", [(i, move(i)) for i in range(n_dp)])


def on_device(
    training_token_input,
    gate_output_gradient,
    up_output_gradient,
    gate_first_matrix,
    gate_second_matrix,
    up_first_matrix,
    up_second_matrix,
    gate_weight_base,
    up_weight_base,
    down_weight_base,
    decode_step_input,
):
    f32, bf16 = jnp.float32, jnp.bfloat16
    n_dp, n_tensor = lax.axis_size("dp"), lax.axis_size("tensor")
    me = lax.axis_index("tensor")
    replica = lax.axis_index("dp")
    rank = gate_first_matrix.shape[1]
    tokens_total = training_token_input.shape[0] * n_dp
    second_learning_rate = 0.5 / math.sqrt(ADAPTER_RANK * tokens_total)
    first_learning_rate = 0.5 / math.sqrt(MODEL_WIDTH * HIDDEN_UNITS * tokens_total / ADAPTER_RANK)
    kernels = n_tensor == 2 and n_dp == 16

    def dot(left, right, over):
        return lax.dot_general(left, right, (over, ((), ())), preferred_element_type=f32)

    firsts = jnp.concatenate([gate_first_matrix, up_first_matrix], axis=1)
    inner = jnp.concatenate(
        [
            jnp.dot(training_token_input, firsts, preferred_element_type=f32),
            dot(gate_output_gradient, gate_second_matrix, ((1,), (1,))),
            dot(up_output_gradient, up_second_matrix, ((1,), (1,))),
        ],
        axis=1,
    )
    inner = pair_sum(inner).astype(bf16)
    inner_b, inner_a = inner[:, : 2 * rank], inner[:, 2 * rank :]

    columns = gate_weight_base.shape[1]
    group = n_dp // n_tensor
    unit = 16 * n_tensor
    padded = -(-columns // unit) * unit
    piece = padded // n_tensor
    second_gradient = jnp.concatenate(
        [
            dot(gate_output_gradient, inner_b[:, :rank], ((0,), (0,))).astype(bf16),
            dot(up_output_gradient, inner_b[:, rank:], ((0,), (0,))).astype(bf16),
        ],
        axis=1,
    )
    second_gradient = jnp.pad(
        second_gradient.reshape(group, columns, 2 * rank),
        ((0, 0), (0, padded - columns), (0, 0)),
    ).reshape(group * padded, 2 * rank)
    rows_in = decode_step_input
    steps = rows_in.shape[0]
    if kernels:
        second_gradient = lax.psum_scatter(second_gradient, "dp", scatter_dimension=0, tiled=True)
        similar = dot(rows_in, training_token_input, ((2,), (1,))).astype(bf16)
        low = jnp.concatenate(
            [dot(similar, inner_a, ((2,), (0,))), dot(rows_in, firsts, ((2,), (0,)))], axis=2
        )
        low = row_share(low, me) + swap(row_share(low, 1 - me).astype(bf16)).astype(f32)
        change = low[..., : 2 * rank]
        moves = [
            lambda i: i ^ 1,
            lambda i: i ^ 2,
            lambda i: i ^ 4,
            lambda i: i ^ 8,
        ]
        for move in moves:
            sent = change.astype(bf16)
            change = sent.astype(f32) + shift_dp(sent, move).astype(f32)
        low = (low[..., 2 * rank :] - first_learning_rate * change).astype(bf16)
    else:
        first_gradient = dot(training_token_input, inner_a, ((0,), (0,))).astype(bf16)
        rows_in, second_gradient, first_gradient = lax.optimization_barrier(
            (rows_in, second_gradient, first_gradient)
        )
        second_gradient = lax.psum_scatter(second_gradient, "dp", scatter_dimension=0, tiled=True)
        first_gradient = lax.psum(first_gradient, "dp")

    def base(rows, weight):
        return dot(rows, weight, ((2,), (0,))).astype(bf16)

    weights = (gate_weight_base, up_weight_base)
    if n_tensor == 2:
        theirs = row_share(rows_in, 1 - me)
        ours = row_share(rows_in, me)
        arrived = [swap(base(theirs, weight)) for weight in weights]
        base_sums = [
            base(ours, weight).astype(f32) + other.astype(f32)
            for weight, other in zip(weights, arrived)
        ]
    else:
        base_sums = [
            lax.psum_scatter(
                base(rows_in, weight), "tensor", scatter_dimension=1, tiled=True
            ).astype(f32)
            for weight in weights
        ]

    start = replica // n_tensor * columns + replica % n_tensor * piece

    def old_piece(matrix):
        wide = jnp.pad(matrix, ((0, 0), (0, padded)))
        return lax.dynamic_slice_in_dim(wide, start, piece, 1).T

    old = jnp.concatenate([old_piece(gate_second_matrix), old_piece(up_second_matrix)], axis=1)
    stepped = (
        old.astype(f32) - second_learning_rate * second_gradient.astype(f32)
    ).astype(bf16)
    routes = [
        (
            (block * n_tensor + part) * n_tensor + side,
            (side * group + block) * n_tensor + part,
        )
        for block in range(group)
        for part in range(n_tensor)
        for side in range(n_tensor)
    ]
    stepped = lax.ppermute(stepped, ("dp", "tensor"), routes)
    if n_tensor == 2:
        other = swap(stepped)
        first_half = me == 0
        seconds = jnp.concatenate(
            [jnp.where(first_half, stepped, other), jnp.where(first_half, other, stepped)], axis=0
        )
    else:
        seconds = lax.all_gather(stepped, "tensor", axis=0, tiled=True)
    seconds = seconds[:columns]

    if not kernels:
        new_firsts = (
            firsts.astype(f32) - first_learning_rate * first_gradient.astype(f32)
        ).astype(bf16)
        low = dot(rows_in, new_firsts, ((2,), (0,)))
        low = lax.psum_scatter(
            low.astype(bf16), "tensor", scatter_dimension=1, tiled=True
        ).astype(bf16)

    gate = base_sums[0] + dot(low[..., :rank], seconds[:, :rank], ((2,), (1,)))
    upper = base_sums[1] + dot(low[..., rank:], seconds[:, rank:], ((2,), (1,)))
    hidden = (jax.nn.silu(gate) * upper).astype(bf16)

    if kernels:
        result = tail(hidden.reshape(-1, columns), down_weight_base, steps)
        return result.reshape(steps, -1, result.shape[1])

    hidden = lax.all_gather(hidden, "tensor", axis=1, tiled=True)
    steps, rows, _ = hidden.shape
    out = dot(hidden, down_weight_base, ((2,), (0,))).astype(bf16)
    out = out.reshape(steps * rows, -1)
    out = lax.psum_scatter(out, "dp", scatter_dimension=0, tiled=True)
    out = lax.all_gather(out, "dp", axis=0, tiled=True)
    return out.reshape(steps, rows, -1)


def solution(mesh):
    placed = (
        P("dp", "tensor"),
        P("dp", "tensor"),
        P("dp", "tensor"),
        P("tensor", None),
        P(None, "tensor"),
        P("tensor", None),
        P(None, "tensor"),
        P("tensor", "dp"),
        P("tensor", "dp"),
        P("dp", "tensor"),
        P(None, None, "tensor"),
    )
    return jax.shard_map(
        on_device, mesh=mesh, in_specs=placed, out_specs=P(None, None, "tensor"), check_vma=False
    )
```

```python
import functools
import math

import jax
import jax.numpy as jnp
from jax import lax
from jax.experimental import pallas as pl
from jax.experimental.pallas import tpu as pltpu
from jax.sharding import PartitionSpec as P

MODEL_WIDTH = 8192
HIDDEN_UNITS = 29568
ADAPTER_RANK = 64
MESH = pl.DeviceIdType.MESH
F32, BF16 = jnp.float32, jnp.bfloat16


def swap(value):
    return lax.ppermute(value, "tensor", ((0, 1), (1, 0)))


def pair_sum(value):
    if lax.axis_size("tensor") == 2:
        sent = value.astype(jnp.bfloat16)
        return sent.astype(jnp.float32) + swap(sent).astype(jnp.float32)
    return lax.psum(value.astype(jnp.bfloat16), "tensor").astype(jnp.float32)


def row_share(value, index):
    rows = value.shape[1] // lax.axis_size("tensor")
    return lax.dynamic_slice_in_dim(value, index * rows, rows, 1)


class Place:
    def __init__(self, n_dp):
        self.chips = n_dp // 2
        depth = self.chips // 2
        dp = lax.axis_index("dp")
        self.t = lax.axis_index("tensor")
        self.core = lax.rem(dp, 2)
        y = lax.rem(dp // 2, 2)
        z = dp // 4
        where = jnp.where(y == 0, z, self.chips - 1 - z)
        self.turn = jnp.where(self.core == 0, where, lax.rem(self.chips - where, self.chips))

        def chip(position):
            position = lax.rem(position + self.chips, self.chips)
            up = position < depth
            there = jnp.where(up, position * 2, (self.chips - 1 - position) * 2 + 1)
            return (there * 2 + self.core, self.t)

        step = jnp.where(self.core == 0, 1, -1)
        self.after = chip(where + step)
        self.before = chip(where - step)
        self.across = (dp, 1 - self.t)
        self.mate = (dp + 1 - 2 * self.core, self.t)
        self.flips = []
        bit = 1
        while bit < n_dp:
            self.flips.append((dp + bit - 2 * bit * lax.rem(dp // bit, 2), self.t))
            bit *= 2


def remote(src, dst, send, recv, target):
    return pltpu.make_async_remote_copy(
        src_ref=src, dst_ref=dst, send_sem=send, recv_sem=recv, device_id=target, device_id_type=MESH
    )


def greet(targets):
    barrier = pltpu.get_barrier_semaphore()
    for target in targets:
        pl.semaphore_signal(barrier, inc=1, device_id=target, device_id_type=MESH)
    pl.semaphore_wait(barrier, len(targets))


def decode_kernel(
    n_dp, steps, inputs_ref, gate_ref, up_ref, down_ref, low_ref, pass_ref, second_ref, first_gate_ref, first_up_ref, out_ref,
    source, piece, own, sent, come, low, passing, passed, second, weight, rows, keep, give, take, ring, result,
    source_sem, piece_sem, small_sem, weight_sem, store_sem, part_send, part_recv, low_send, low_recv, across_send, across_recv,
    mate_send, mate_recv, sum_send, sum_recv, all_send, all_recv, copy_send, copy_recv,
):
    place = Place(n_dp)
    n = place.chips
    chunks = rows.shape[0]
    per = chunks // steps
    share = source.shape[1]
    part = share // per
    units = rows.shape[2]
    half = weight.shape[1] // 2
    shard = 2 * part // n
    tile = min(512, half)
    tiles = half // tile
    spans = [(i, min(piece.shape[1], units - i)) for i in range(0, units, piece.shape[1])]
    mine = pl.multiple_of(place.core * half, half)
    other = pl.multiple_of((1 - place.core) * half, half)

    groups = [(0, place.t), (1, 1 - place.t), (1, place.t)]
    turns = [(g, m, span) for g in range(len(groups)) for m in range(2) for span in spans]

    def source_copy(g):
        step, side = groups[g]
        first = pl.multiple_of(step * 2 * share + side * share, share)
        return pltpu.make_async_copy(inputs_ref.at[pl.ds(first, share), :], source.at[g % 2], source_sem.at[g % 2])

    def piece_copy(i):
        _, m, (first, width) = turns[i]
        ref = (gate_ref, up_ref)[m]
        return pltpu.make_async_copy(
            ref.at[pl.ds(first, width), :], piece.at[i % 2, pl.ds(0, width), :], piece_sem.at[i % 2]
        )

    smalls = [
        pltpu.make_async_copy(low_ref, low, small_sem.at[0]),
        pltpu.make_async_copy(second_ref, second, small_sem.at[1]),
        pltpu.make_async_copy(first_gate_ref, come.at[0, 0], small_sem.at[2]),
        pltpu.make_async_copy(first_up_ref, come.at[0, 1], small_sem.at[3]),
        pltpu.make_async_copy(pass_ref, passing, small_sem.at[4]),
    ]
    low_copy = remote(passing, passed, low_send.at[0], low_recv.at[0], place.across)
    weight_load = pltpu.make_async_copy(down_ref, weight, weight_sem.at[0])

    source_copy(0).start()
    piece_copy(0).start()
    piece_copy(1).start()
    source_copy(1).start()
    for small in smalls:
        small.start()
    greet((place.across, place.mate, place.after, place.before))
    for small in smalls:
        small.wait()
    low_copy.start()

    def base(g):
        for i, (group, m, (first, width)) in enumerate(turns):
            if group != g:
                continue
            if m == 0 and first == 0:
                source_copy(g).wait()
            piece_copy(i).wait()
            columns = pl.ds(first, width)
            value = lax.dot_general(
                source[g % 2], piece[i % 2, :width, :], (((1,), (1,)), ((), ())), preferred_element_type=F32
            ).astype(BF16)
            if g == 1:
                sent[m, :, columns] = value
            else:
                own[groups[g][0], m, :, columns] = value
            if i + 2 < len(turns):
                piece_copy(i + 2).start()
            if m == 1 and (first, width) == spans[-1] and g + 2 < len(groups):
                source_copy(g + 2).start()
            yield

    def partial_copies(q):
        here = pl.ds((q % per) * part, part)
        return [
            remote(sent.at[m, here, :], come.at[1, m, here, :], part_send.at[q % per, m], part_recv.at[q % per, m], place.across)
            for m in range(2)
        ]

    def own_rows(q):
        return rows.at[q, pl.ds(pl.multiple_of(place.t * part, part), part), :]

    def crossing(q):
        return remote(own_rows(q), own_rows(q), across_send.at[q], across_recv.at[q], place.across)

    def hidden(q):
        step = q // per
        count = 64
        for i in range(part // count):
            here = pl.ds((q % per) * part + i * count, count)
            line = pl.ds(q * part + i * count, count)
            there = pl.ds(pl.multiple_of(place.t * part + i * count, count), count)
            for first, width in spans:
                columns = pl.ds(first, width)

                def pre(m):
                    return (
                        own[step, m, here, columns].astype(F32) + come[step, m, here, columns].astype(F32)
                        + jnp.dot(low[m, line, :], second[m, :, columns], preferred_element_type=F32)
                    )

                gate = pre(0)
                rows[q, there, columns] = (gate / (1.0 + jnp.exp(-gate)) * pre(1)).astype(BF16)
        crossing(q).start()

    def shard_rows(index):
        index = lax.rem(index + 2 * n, n)
        return pl.ds(pl.multiple_of(index * shard, shard), shard)

    def product(q, i, target, start):
        block = pl.ds(pl.multiple_of(start + i * tile, tile), tile)
        value = jnp.dot(rows[q], weight[:, block], preferred_element_type=F32)
        target[q, :, pl.ds(i * tile, tile)] = value.astype(BF16)

    pending = []

    def project(q):
        crossing(q).wait_recv()
        exchange = remote(give.at[q], take.at[q], mate_send.at[q], mate_recv.at[q], place.mate)
        for i in range(tiles):
            product(q, i, give, other)
            if i == tiles - 1:
                exchange.start()
            yield
        for i in range(tiles):
            product(q, i, keep, mine)
            yield
        exchange.wait()

    up, down = n // 2, n - 1 - n // 2
    ways = ((0, up, place.after), (1, down, place.before))

    def spread(q):
        hops = [None, None]

        def mix(where):
            return keep[q, where, :].astype(F32) + take[q, where, :].astype(F32)

        for s in range(up):
            for d, count, there in ways:
                if s < count:
                    where = shard_rows(place.turn + (up - s if d == 0 else s - down))
                    value = mix(where)
                    if s > 0:
                        hops[d].wait()
                        value = value + ring[q, d * up + s - 1].astype(F32)
                    keep[q, where, :] = value.astype(BF16)
                    slot = d * up + s
                    hops[d] = remote(
                        keep.at[q, where, :], ring.at[q, slot], sum_send.at[q, slot], sum_recv.at[q, slot], there
                    )
                    hops[d].start()
            yield
        where = shard_rows(place.turn)
        value = mix(where)
        for d, count, there in ways:
            hops[d].wait()
            value = value + ring[q, d * up + count - 1].astype(F32)
        result[q, where, pl.ds(mine, half)] = value.astype(BF16)
        copies = []
        for s in range(up + 1):
            for d, count, there in ways:
                if s > count:
                    continue
                if s > 0:
                    hops[d].wait()
                block = result.at[q, shard_rows(place.turn + (-s if d == 0 else s)), pl.ds(mine, half)]
                if s < count:
                    slot = d * up + s
                    hops[d] = remote(block, block, all_send.at[q, slot], all_recv.at[q, slot], there)
                    hops[d].start()
                if s > 0 or d == 0:
                    slot = d * up + s
                    copy = remote(block, block, copy_send.at[q, slot], copy_recv.at[q, slot], place.mate)
                    copy.start()
                    copies.append(copy)
            yield
        for copy in copies:
            copy.wait()
        for side in range(2):
            first = (q // per) * 2 * share + side * share + (q % per) * part
            store = pltpu.make_async_copy(
                result.at[q, pl.ds(side * part, part), :], out_ref.at[pl.ds(first, part), :], store_sem.at[q, side]
            )
            store.start()
            pending.append(store)

    for _ in base(0):
        pass
    weight_load.start()
    low_copy.wait()
    low[...] = (low[...].astype(F32) + passed[...].astype(F32)).astype(BF16)
    hidden(0)
    hidden(1)
    for _ in base(1):
        pass
    for copy in partial_copies(2):
        copy.start()
    weight_load.wait()
    for _ in project(0):
        pass
    live = {0: spread(0)}

    def paced(units, count):
        for i, _ in enumerate(units):
            if i % count == count - 1:
                yield

    def background():
        yield
        for _ in project(1):
            pass
        live[1] = spread(1)
        yield
        yield from paced(base(2), 6)
        for copy in partial_copies(2):
            copy.wait_recv()
        hidden(2)
        for copy in partial_copies(3):
            copy.start()
        yield
        yield
        yield from paced(project(2), 4)
        live[2] = spread(2)
        yield
        yield
        for copy in partial_copies(3):
            copy.wait_recv()
        hidden(3)
        yield
        yield
        for _ in project(3):
            pass
        live[3] = spread(3)

    rest = background()
    busy = True
    while busy or live:
        for q in list(live):
            if next(live[q], live) is live:
                del live[q]
        if busy and next(rest, live) is live:
            busy = False
    for store in pending:
        store.wait()
    for q in range(chunks):
        crossing(q).wait_send()
    for q in range(per, chunks):
        for copy in partial_copies(q):
            copy.wait_send()


def decode(inputs, gate, up, down, low, passing, second, first_gate, first_up, steps):
    n_dp = lax.axis_size("dp")
    n = n_dp // 2
    count, features = inputs.shape
    units, width = down.shape
    chunks = 2 * steps
    share = count // (2 * steps)
    both = count // chunks
    rank = low.shape[2]
    dma = pltpu.SemaphoreType.DMA
    anywhere = pl.BlockSpec(memory_space=pl.ANY)
    return pl.pallas_call(
        functools.partial(decode_kernel, n_dp, steps),
        out_shape=jax.ShapeDtypeStruct((count, width), BF16),
        in_specs=[anywhere] * 9,
        out_specs=anywhere,
        scratch_shapes=[
            pltpu.VMEM((2, share, features), BF16),
            pltpu.VMEM((2, 256, features), BF16),
            pltpu.VMEM((steps, 2, share, units), BF16),
            pltpu.VMEM((2, share, units), BF16),
            pltpu.VMEM((steps, 2, share, units), BF16),
            pltpu.VMEM(low.shape, BF16),
            pltpu.VMEM(low.shape, BF16),
            pltpu.VMEM(low.shape, BF16),
            pltpu.VMEM((2, rank, units), BF16),
            pltpu.VMEM((units, width), BF16),
            pltpu.VMEM((chunks, both, units), BF16),
            pltpu.VMEM((chunks, both, width // 2), BF16),
            pltpu.VMEM((chunks, both, width // 2), BF16),
            pltpu.VMEM((chunks, both, width // 2), BF16),
            pltpu.VMEM((chunks, n - 1, both // n, width // 2), BF16),
            pltpu.VMEM((chunks, both, width), BF16),
            dma((2,)), dma((2,)), dma((5,)), dma((1,)), dma((chunks, 2)),
            dma((2, 2)), dma((2, 2)), dma((1,)), dma((1,)), dma((chunks,)), dma((chunks,)), dma((chunks,)), dma((chunks,)),
            dma((chunks, n)), dma((chunks, n)), dma((chunks, n)), dma((chunks, n)),
            dma((chunks, n)), dma((chunks, n)),
        ],
        compiler_params=pltpu.CompilerParams(
            collective_id=0, has_side_effects=True, vmem_limit_bytes=63 * 1024 * 1024
        ),
        name="decode",
    )(inputs, gate, up, down, low, passing, second, first_gate, first_up)


def seconds_kernel(
    n_dp, n_tensor, rate, gate_ref, up_ref, old_ref, change_ref, out_ref, change_out_ref,
    change, summed, heard, whole, raw, block, take, ring, old, fresh,
    load_sem, old_sem, store_sem, mate_send, mate_recv, ring_send, ring_recv, across_send, across_recv,
    change_sem, hear_send, hear_recv,
):
    place = Place(n_dp)
    n = place.chips
    depth = n // 2
    rank = raw.shape[1]
    units = block.shape[2]
    kept = n // n_tensor
    cuts = ring_send.shape[2]
    cut = 2 * rank // cuts

    loads = [pltpu.make_async_copy(ref, raw.at[p], load_sem.at[p]) for p, ref in enumerate((gate_ref, up_ref))]
    for load in loads:
        load.start()
    held = pltpu.make_async_copy(old_ref, old, old_sem.at[0])
    held.start()
    change_load = pltpu.make_async_copy(change_ref, change, change_sem.at[0])
    change_load.start()
    greet((place.across, place.mate, place.after, place.before) + tuple(place.flips[1:]))
    change_load.wait()
    rounds = len(place.flips)

    lines = heard.shape[1]

    def hear(i):
        if i == 0:
            src = change.at[pl.ds(pl.multiple_of((1 - place.core) * lines, lines), lines), :]
        else:
            src = summed.at[i - 1]
        return remote(src, heard.at[i], hear_send.at[i], hear_recv.at[i], place.flips[i])

    def gather(i):
        hear(i).wait()
        mine = pl.ds(pl.multiple_of(place.core * lines, lines), lines)
        before = change[mine, :] if i == 0 else summed[i - 1]
        value = (before.astype(F32) + heard[i].astype(F32)).astype(BF16)
        if i + 1 < rounds:
            summed[i] = value
            hear(i + 1).start()
        else:
            whole[mine, :] = value

    def complete():
        mine = pl.ds(pl.multiple_of(place.core * lines, lines), lines)
        return remote(whole.at[mine, :], whole.at[mine, :], hear_send.at[rounds], hear_recv.at[rounds], place.mate)

    hear(0).start()
    for load in loads:
        load.wait()

    exchanges = []
    for j in range(kept):
        for k in (2 * j, 2 * j + 1):
            for p in range(2):
                block[k, p * rank : (p + 1) * rank, :] = raw[p, :, k * units : (k + 1) * units]
        exchange = remote(
            block.at[2 * j + 1 - place.core], take.at[j], mate_send.at[j], mate_recv.at[j], place.mate
        )
        exchange.start()
        exchanges.append(exchange)
    gather(0)
    for exchange in exchanges:
        exchange.wait()
    held.wait()

    def target(index):
        index = lax.rem(index + 2 * n, n)
        where = jnp.where(place.core == 0, index, lax.rem(n - index, n))
        y = jnp.where(where < depth, 0, 1)
        z = jnp.where(where < depth, where, n - 1 - where)
        per = depth // n_tensor
        return z // per == place.t, lax.rem(z, per) * 2 + y

    def hop(d, j, u):
        own = pl.ds(u * cut, cut)
        return remote(
            block.at[2 * j + place.core, own, :], ring.at[d, j, own, :],
            ring_send.at[d, j, u], ring_recv.at[d, j, u], (place.after, place.before)[d],
        )

    def final(u):
        own = pl.ds(u * cut, cut)
        return remote(fresh.at[own, :], fresh.at[own, :], across_send.at[u], across_recv.at[u], place.across)

    up, down = n // 2, n - 1 - n // 2
    sends = [
        (s, d, target(place.turn + (up - s if d == 0 else s - down)))
        for s in range(up) for d, count in ((0, up), (1, down)) if s < count
    ]

    def mix(j, u):
        own = pl.ds(u * cut, cut)
        return block[2 * j + place.core, own, :].astype(F32) + take[j, own, :].astype(F32)

    for s, d, (active, j) in sends:

        @pl.when(active)
        def _():
            for u in range(cuts):
                own = pl.ds(u * cut, cut)
                value = mix(j, u)
                if s > 0:
                    hop(d, j, u).wait_recv()
                    value = value + ring[d, j, own, :].astype(F32)
                block[2 * j + place.core, own, :] = value.astype(BF16)
                hop(d, j, u).start()

        if d == 0 and 1 <= s < rounds - 1:
            gather(s)

    owner, j = target(place.turn)

    @pl.when(owner)
    def _():
        for u in range(cuts):
            own = pl.ds(u * cut, cut)
            value = mix(j, u)
            for d in range(2):
                hop(d, j, u).wait_recv()
                value = value + ring[d, j, own, :].astype(F32)
            fresh[own, :] = (old[own, :].astype(F32) - rate * value).astype(BF16)
            final(u).start()

    gather(rounds - 1)
    complete().start()
    for s, d, (active, j) in sends:

        @pl.when(active)
        def _():
            for u in range(cuts):
                hop(d, j, u).wait_send()

    @pl.when(owner)
    def _():
        for u in range(cuts):
            final(u).wait_send()

    @pl.when(jnp.logical_not(owner))
    def _():
        for u in range(cuts):
            final(u).wait_recv()

    complete().wait()
    stores = [
        pltpu.make_async_copy(fresh, out_ref, store_sem.at[0]),
        pltpu.make_async_copy(whole, change_out_ref, change_sem.at[1]),
    ]
    for store in stores:
        store.start()
    for store in stores:
        store.wait()


def new_seconds(gate_gradient, up_gradient, old, change, rate):
    rounds = 4
    n_dp, n_tensor = lax.axis_size("dp"), lax.axis_size("tensor")
    both, units = old.shape
    n = n_dp // 2
    kept, cuts = n // n_tensor, 4
    dma = pltpu.SemaphoreType.DMA
    anywhere = pl.BlockSpec(memory_space=pl.ANY)
    return pl.pallas_call(
        functools.partial(seconds_kernel, n_dp, n_tensor, rate),
        out_shape=(jax.ShapeDtypeStruct((both, units), BF16), jax.ShapeDtypeStruct(change.shape, BF16)),
        in_specs=[anywhere] * 4,
        out_specs=(anywhere, anywhere),
        scratch_shapes=[
            pltpu.VMEM(change.shape, BF16),
            pltpu.VMEM((rounds - 1, change.shape[0] // 2, both), BF16),
            pltpu.VMEM((rounds, change.shape[0] // 2, both), BF16),
            pltpu.VMEM(change.shape, BF16),
            pltpu.VMEM((2, both // 2, gate_gradient.shape[1]), BF16),
            pltpu.VMEM((2 * kept, both, units), BF16),
            pltpu.VMEM((kept, both, units), BF16),
            pltpu.VMEM((2, kept, both, units), BF16),
            pltpu.VMEM((both, units), BF16),
            pltpu.VMEM((both, units), BF16),
            dma((2,)), dma((1,)), dma((1,)),
            dma((kept,)), dma((kept,)), dma((2, kept, cuts)), dma((2, kept, cuts)), dma((cuts,)), dma((cuts,)),
            dma((2,)), dma((rounds + 1,)), dma((rounds + 1,)),
        ],
        compiler_params=pltpu.CompilerParams(
            collective_id=1, has_side_effects=True, vmem_limit_bytes=28 * 1024 * 1024
        ),
        cost_estimate=pl.CostEstimate(flops=0, bytes_accessed=100_000_000, transcendentals=0),
        name="seconds",
    )(gate_gradient, up_gradient, old, change)


def on_device(
    training_token_input,
    gate_output_gradient,
    up_output_gradient,
    gate_first_matrix,
    gate_second_matrix,
    up_first_matrix,
    up_second_matrix,
    gate_weight_base,
    up_weight_base,
    down_weight_base,
    decode_step_input,
):
    f32, bf16 = jnp.float32, jnp.bfloat16
    n_dp, n_tensor = lax.axis_size("dp"), lax.axis_size("tensor")
    me = lax.axis_index("tensor")
    replica = lax.axis_index("dp")
    rank = gate_first_matrix.shape[1]
    tokens_total = training_token_input.shape[0] * n_dp
    second_learning_rate = 0.5 / math.sqrt(ADAPTER_RANK * tokens_total)
    first_learning_rate = 0.5 / math.sqrt(MODEL_WIDTH * HIDDEN_UNITS * tokens_total / ADAPTER_RANK)
    kernels = n_tensor == 2 and n_dp == 16 and decode_step_input.shape[0] == 2

    def dot(left, right, over):
        return lax.dot_general(left, right, (over, ((), ())), preferred_element_type=f32)

    firsts = jnp.concatenate([gate_first_matrix, up_first_matrix], axis=1)
    inner = jnp.concatenate(
        [
            jnp.dot(training_token_input, firsts, preferred_element_type=f32),
            dot(gate_output_gradient, gate_second_matrix, ((1,), (1,))),
            dot(up_output_gradient, up_second_matrix, ((1,), (1,))),
        ],
        axis=1,
    )
    inner, rows_in = lax.optimization_barrier((inner.astype(bf16), decode_step_input))
    inner = pair_sum(inner).astype(bf16)
    inner_b, inner_a = inner[:, : 2 * rank], inner[:, 2 * rank :]

    columns = gate_weight_base.shape[1]
    group = n_dp // n_tensor
    steps = rows_in.shape[0]
    if kernels:
        theirs = row_share(rows_in, 1 - me)[0]
        arrived = [
            swap(jnp.dot(theirs, weight, preferred_element_type=f32).astype(bf16))
            for weight in (gate_weight_base, up_weight_base)
        ]
        similar = dot(rows_in, training_token_input, ((2,), (1,))).astype(bf16)
        change = dot(similar, inner_a, ((2,), (0,))).astype(bf16)
        block = lax.rem(replica, group)

        def old_block(matrix):
            return lax.dynamic_slice_in_dim(matrix, block * columns, columns, 1)

        seconds, change = new_seconds(
            dot(inner_b[:, :rank], gate_output_gradient, ((0,), (0,))).astype(bf16),
            dot(inner_b[:, rank:], up_output_gradient, ((0,), (0,))).astype(bf16),
            jnp.concatenate([old_block(gate_second_matrix), old_block(up_second_matrix)], axis=0),
            change.reshape(-1, 2 * rank),
            second_learning_rate,
        )
        low = dot(rows_in, firsts, ((2,), (0,))) - first_learning_rate * change.reshape(
            steps, -1, 2 * rank
        ).astype(f32)
    else:
        unit = 16 * n_tensor
        padded = -(-columns // unit) * unit
        piece = padded // n_tensor
        second_gradient = jnp.concatenate(
            [
                dot(gate_output_gradient, inner_b[:, :rank], ((0,), (0,))).astype(bf16),
                dot(up_output_gradient, inner_b[:, rank:], ((0,), (0,))).astype(bf16),
            ],
            axis=1,
        )
        second_gradient = jnp.pad(
            second_gradient.reshape(group, columns, 2 * rank),
            ((0, 0), (0, padded - columns), (0, 0)),
        ).reshape(group * padded, 2 * rank)
        first_gradient = dot(training_token_input, inner_a, ((0,), (0,))).astype(bf16)
        rows_in, second_gradient, first_gradient = lax.optimization_barrier(
            (rows_in, second_gradient, first_gradient)
        )
        second_gradient = lax.psum_scatter(second_gradient, "dp", scatter_dimension=0, tiled=True)
        first_gradient = lax.psum(first_gradient, "dp")
        start = replica // n_tensor * columns + replica % n_tensor * piece

        def old_piece(matrix):
            wide = jnp.pad(matrix, ((0, 0), (0, padded)))
            return lax.dynamic_slice_in_dim(wide, start, piece, 1).T

        old = jnp.concatenate([old_piece(gate_second_matrix), old_piece(up_second_matrix)], axis=1)
        stepped = (
            old.astype(f32) - second_learning_rate * second_gradient.astype(f32)
        ).astype(bf16)
        routes = [
            (
                (block * n_tensor + part) * n_tensor + side,
                (side * group + block) * n_tensor + part,
            )
            for block in range(group)
            for part in range(n_tensor)
            for side in range(n_tensor)
        ]
        stepped = lax.ppermute(stepped, ("dp", "tensor"), routes)
        seconds = lax.all_gather(stepped, "tensor", axis=0, tiled=True)[:columns].T
        new_firsts = (
            firsts.astype(f32) - first_learning_rate * first_gradient.astype(f32)
        ).astype(bf16)
        low = dot(rows_in, new_firsts, ((2,), (0,)))
        low = lax.psum_scatter(
            low.astype(bf16), "tensor", scatter_dimension=1, tiled=True
        ).astype(bf16)

    def base(rows, weight):
        return dot(rows, weight, ((2,), (0,))).astype(bf16)

    weights = (gate_weight_base, up_weight_base)
    if kernels:

        def share_of(side):
            value = row_share(low, side).astype(bf16).reshape(-1, 2 * rank)
            return jnp.stack([value[:, :rank], value[:, rank:]])

        result = decode(
            rows_in.reshape(-1, rows_in.shape[2]),
            gate_weight_base.T,
            up_weight_base.T,
            down_weight_base,
            share_of(me),
            share_of(1 - me),
            seconds.reshape(2, rank, columns),
            *arrived,
            steps,
        )
        return result.reshape(steps, -1, result.shape[1])

    base_sums = [
        lax.psum_scatter(
            base(rows_in, weight), "tensor", scatter_dimension=1, tiled=True
        ).astype(f32)
        for weight in weights
    ]
    gate = base_sums[0] + dot(low[..., :rank], seconds[:rank], ((2,), (0,)))
    upper = base_sums[1] + dot(low[..., rank:], seconds[rank:], ((2,), (0,)))
    hidden = (jax.nn.silu(gate) * upper).astype(bf16)

    hidden = lax.all_gather(hidden, "tensor", axis=1, tiled=True)
    steps, rows, _ = hidden.shape
    out = dot(hidden, down_weight_base, ((2,), (0,))).astype(bf16)
    out = out.reshape(steps * rows, -1)
    out = lax.psum_scatter(out, "dp", scatter_dimension=0, tiled=True)
    out = lax.all_gather(out, "dp", axis=0, tiled=True)
    return out.reshape(steps, rows, -1)


def solution(mesh):
    placed = (
        P("dp", "tensor"),
        P("dp", "tensor"),
        P("dp", "tensor"),
        P("tensor", None),
        P(None, "tensor"),
        P("tensor", None),
        P(None, "tensor"),
        P("tensor", "dp"),
        P("tensor", "dp"),
        P("dp", "tensor"),
        P(None, None, "tensor"),
    )
    return jax.shard_map(
        on_device, mesh=mesh, in_specs=placed, out_specs=P(None, None, "tensor"), check_vma=False
    )
```

```python
import functools
import math

import jax
import jax.numpy as jnp
from jax import lax
from jax.experimental import pallas as pl
from jax.experimental.pallas import tpu as pltpu
from jax.sharding import PartitionSpec as P

MODEL_WIDTH = 8192
HIDDEN_UNITS = 29568
ADAPTER_RANK = 64
MESH = pl.DeviceIdType.MESH
F32, BF16 = jnp.float32, jnp.bfloat16


def swap(value):
    return lax.ppermute(value, "tensor", ((0, 1), (1, 0)))


def pair_sum(value):
    if lax.axis_size("tensor") == 2:
        sent = value.astype(jnp.bfloat16)
        return sent.astype(jnp.float32) + swap(sent).astype(jnp.float32)
    return lax.psum(value.astype(jnp.bfloat16), "tensor").astype(jnp.float32)


def row_share(value, index):
    rows = value.shape[1] // lax.axis_size("tensor")
    return lax.dynamic_slice_in_dim(value, index * rows, rows, 1)


class Place:
    def __init__(self, n_dp):
        self.chips = n_dp // 2
        depth = self.chips // 2
        dp = lax.axis_index("dp")
        self.t = lax.axis_index("tensor")
        self.core = lax.rem(dp, 2)
        y = lax.rem(dp // 2, 2)
        z = dp // 4
        where = jnp.where(y == 0, z, self.chips - 1 - z)
        self.turn = jnp.where(self.core == 0, where, lax.rem(self.chips - where, self.chips))

        def chip(position):
            position = lax.rem(position + self.chips, self.chips)
            up = position < depth
            there = jnp.where(up, position * 2, (self.chips - 1 - position) * 2 + 1)
            return (there * 2 + self.core, self.t)

        step = jnp.where(self.core == 0, 1, -1)
        self.after = chip(where + step)
        self.before = chip(where - step)
        self.across = (dp, 1 - self.t)
        self.mate = (dp + 1 - 2 * self.core, self.t)
        self.flips = []
        bit = 1
        while bit < n_dp:
            self.flips.append((dp + bit - 2 * bit * lax.rem(dp // bit, 2), self.t))
            bit *= 2


def remote(src, dst, send, recv, target):
    return pltpu.make_async_remote_copy(
        src_ref=src, dst_ref=dst, send_sem=send, recv_sem=recv, device_id=target, device_id_type=MESH
    )


def greet(targets):
    barrier = pltpu.get_barrier_semaphore()
    for target in targets:
        pl.semaphore_signal(barrier, inc=1, device_id=target, device_id_type=MESH)
    pl.semaphore_wait(barrier, len(targets))


def decode_kernel(
    n_dp, steps, inputs_ref, gate_ref, up_ref, down_ref, low_ref, pass_ref, second_ref, first_gate_ref, first_up_ref, out_ref,
    source, piece, own, sent, come, low, passing, passed, second, weight, rows, keep, give, take, ring, result,
    source_sem, piece_sem, small_sem, weight_sem, store_sem, part_send, part_recv, low_send, low_recv, across_send, across_recv,
    mate_send, mate_recv, sum_send, sum_recv, all_send, all_recv, copy_send, copy_recv,
):
    place = Place(n_dp)
    n = place.chips
    chunks = rows.shape[0]
    per = chunks // steps
    share = source.shape[1]
    part = share // per
    units = rows.shape[2]
    half = weight.shape[1] // 2
    shard = 2 * part // n
    tile = min(512, half)
    tiles = half // tile
    spans = [(i, min(piece.shape[1], units - i)) for i in range(0, units, piece.shape[1])]
    mine = pl.multiple_of(place.core * half, half)
    other = pl.multiple_of((1 - place.core) * half, half)

    groups = [(0, place.t), (1, 1 - place.t), (1, place.t)]
    turns = [(g, m, span) for g in range(len(groups)) for m in range(2) for span in spans]

    def source_copy(g):
        step, side = groups[g]
        first = pl.multiple_of(step * 2 * share + side * share, share)
        return pltpu.make_async_copy(inputs_ref.at[pl.ds(first, share), :], source.at[g % 2], source_sem.at[g % 2])

    def piece_copy(i):
        _, m, (first, width) = turns[i]
        ref = (gate_ref, up_ref)[m]
        return pltpu.make_async_copy(
            ref.at[pl.ds(first, width), :], piece.at[i % 2, pl.ds(0, width), :], piece_sem.at[i % 2]
        )

    smalls = [
        pltpu.make_async_copy(low_ref, low, small_sem.at[0]),
        pltpu.make_async_copy(second_ref, second, small_sem.at[1]),
        pltpu.make_async_copy(first_gate_ref, come.at[0, 0], small_sem.at[2]),
        pltpu.make_async_copy(first_up_ref, come.at[0, 1], small_sem.at[3]),
        pltpu.make_async_copy(pass_ref, passing, small_sem.at[4]),
    ]
    low_copy = remote(passing, passed, low_send.at[0], low_recv.at[0], place.across)
    weight_load = pltpu.make_async_copy(down_ref, weight, weight_sem.at[0])

    source_copy(0).start()
    piece_copy(0).start()
    piece_copy(1).start()
    source_copy(1).start()
    for small in smalls:
        small.start()
    greet((place.across, place.mate, place.after, place.before))
    for small in smalls:
        small.wait()
    low_copy.start()

    def base(g):
        for i, (group, m, (first, width)) in enumerate(turns):
            if group != g:
                continue
            if m == 0 and first == 0:
                source_copy(g).wait()
            piece_copy(i).wait()
            columns = pl.ds(first, width)
            value = lax.dot_general(
                source[g % 2], piece[i % 2, :width, :], (((1,), (1,)), ((), ())), preferred_element_type=F32
            ).astype(BF16)
            if g == 1:
                sent[m, :, columns] = value
            else:
                own[groups[g][0], m, :, columns] = value
            if i + 2 < len(turns):
                piece_copy(i + 2).start()
            if m == 1 and (first, width) == spans[-1] and g + 2 < len(groups):
                source_copy(g + 2).start()
            yield

    def partial_copies(q):
        here = pl.ds((q % per) * part, part)
        return [
            remote(sent.at[m, here, :], come.at[1, m, here, :], part_send.at[q % per, m], part_recv.at[q % per, m], place.across)
            for m in range(2)
        ]

    def own_rows(q):
        return rows.at[q, pl.ds(pl.multiple_of(place.t * part, part), part), :]

    def crossing(q):
        return remote(own_rows(q), own_rows(q), across_send.at[q], across_recv.at[q], place.across)

    def hidden(q):
        step = q // per
        count = 64
        for i in range(part // count):
            here = pl.ds((q % per) * part + i * count, count)
            line = pl.ds(q * part + i * count, count)
            there = pl.ds(pl.multiple_of(place.t * part + i * count, count), count)
            for first, width in spans:
                columns = pl.ds(first, width)

                def pre(m):
                    return (
                        own[step, m, here, columns].astype(F32) + come[step, m, here, columns].astype(F32)
                        + jnp.dot(low[m, line, :], second[m, :, columns], preferred_element_type=F32)
                    )

                gate = pre(0)
                rows[q, there, columns] = (gate / (1.0 + jnp.exp(-gate)) * pre(1)).astype(BF16)
        crossing(q).start()

    def shard_rows(index):
        index = lax.rem(index + 2 * n, n)
        return pl.ds(pl.multiple_of(index * shard, shard), shard)

    def product(q, i, target, start):
        block = pl.ds(pl.multiple_of(start + i * tile, tile), tile)
        value = jnp.dot(rows[q], weight[:, block], preferred_element_type=F32)
        target[q, :, pl.ds(i * tile, tile)] = value.astype(BF16)

    pending = []

    def project(q):
        crossing(q).wait_recv()
        exchange = remote(give.at[q], take.at[q], mate_send.at[q], mate_recv.at[q], place.mate)
        for i in range(tiles):
            product(q, i, give, other)
            if i == tiles - 1:
                exchange.start()
            yield
        for i in range(tiles):
            product(q, i, keep, mine)
            yield
        exchange.wait()

    up, down = n // 2, n - 1 - n // 2
    ways = ((0, up, place.after), (1, down, place.before))

    def spread(q):
        hops = [None, None]

        def mix(where):
            return keep[q, where, :].astype(F32) + take[q, where, :].astype(F32)

        for s in range(up):
            for d, count, there in ways:
                if s < count:
                    where = shard_rows(place.turn + (up - s if d == 0 else s - down))
                    value = mix(where)
                    if s > 0:
                        hops[d].wait()
                        value = value + ring[q, d * up + s - 1].astype(F32)
                    keep[q, where, :] = value.astype(BF16)
                    slot = d * up + s
                    hops[d] = remote(
                        keep.at[q, where, :], ring.at[q, slot], sum_send.at[q, slot], sum_recv.at[q, slot], there
                    )
                    hops[d].start()
            yield
        where = shard_rows(place.turn)
        value = mix(where)
        for d, count, there in ways:
            hops[d].wait()
            value = value + ring[q, d * up + count - 1].astype(F32)
        result[q, where, pl.ds(mine, half)] = value.astype(BF16)
        copies = []
        for s in range(up + 1):
            for d, count, there in ways:
                if s > count:
                    continue
                if s > 0:
                    hops[d].wait()
                block = result.at[q, shard_rows(place.turn + (-s if d == 0 else s)), pl.ds(mine, half)]
                if s < count:
                    slot = d * up + s
                    hops[d] = remote(block, block, all_send.at[q, slot], all_recv.at[q, slot], there)
                    hops[d].start()
                if s > 0 or d == 0:
                    slot = d * up + s
                    copy = remote(block, block, copy_send.at[q, slot], copy_recv.at[q, slot], place.mate)
                    copy.start()
                    copies.append(copy)
            yield
        for copy in copies:
            copy.wait()
        for side in range(2):
            first = (q // per) * 2 * share + side * share + (q % per) * part
            store = pltpu.make_async_copy(
                result.at[q, pl.ds(side * part, part), :], out_ref.at[pl.ds(first, part), :], store_sem.at[q, side]
            )
            store.start()
            pending.append(store)

    for _ in base(0):
        pass
    weight_load.start()
    low_copy.wait()
    low[...] = (low[...].astype(F32) + passed[...].astype(F32)).astype(BF16)
    hidden(0)
    hidden(1)
    for _ in base(1):
        pass
    for copy in partial_copies(2) + partial_copies(3):
        copy.start()
    weight_load.wait()
    for _ in project(0):
        pass
    live = {0: spread(0)}

    def paced(units, count):
        for i, _ in enumerate(units):
            if i % count == count - 1:
                yield

    def background():
        yield from paced(base(2), 6)
        yield from paced(project(1), 3)
        live[1] = spread(1)
        yield
        for copy in partial_copies(2):
            copy.wait_recv()
        hidden(2)
        yield
        yield from paced(project(2), 3)
        live[2] = spread(2)
        yield
        for copy in partial_copies(3):
            copy.wait_recv()
        hidden(3)
        yield
        yield from paced(project(3), 3)
        live[3] = spread(3)

    rest = background()
    busy = True
    while busy or live:
        for q in list(live):
            if next(live[q], live) is live:
                del live[q]
        if busy and next(rest, live) is live:
            busy = False
    for store in pending:
        store.wait()
    for q in range(chunks):
        crossing(q).wait_send()
    for q in range(per, chunks):
        for copy in partial_copies(q):
            copy.wait_send()


def decode(inputs, gate, up, down, low, passing, second, first_gate, first_up, steps):
    n_dp = lax.axis_size("dp")
    n = n_dp // 2
    count, features = inputs.shape
    units, width = down.shape
    chunks = 2 * steps
    share = count // (2 * steps)
    both = count // chunks
    rank = low.shape[2]
    dma = pltpu.SemaphoreType.DMA
    anywhere = pl.BlockSpec(memory_space=pl.ANY)
    return pl.pallas_call(
        functools.partial(decode_kernel, n_dp, steps),
        out_shape=jax.ShapeDtypeStruct((count, width), BF16),
        in_specs=[anywhere] * 9,
        out_specs=anywhere,
        scratch_shapes=[
            pltpu.VMEM((2, share, features), BF16),
            pltpu.VMEM((2, 256, features), BF16),
            pltpu.VMEM((steps, 2, share, units), BF16),
            pltpu.VMEM((2, share, units), BF16),
            pltpu.VMEM((steps, 2, share, units), BF16),
            pltpu.VMEM(low.shape, BF16),
            pltpu.VMEM(low.shape, BF16),
            pltpu.VMEM(low.shape, BF16),
            pltpu.VMEM((2, rank, units), BF16),
            pltpu.VMEM((units, width), BF16),
            pltpu.VMEM((chunks, both, units), BF16),
            pltpu.VMEM((chunks, both, width // 2), BF16),
            pltpu.VMEM((chunks, both, width // 2), BF16),
            pltpu.VMEM((chunks, both, width // 2), BF16),
            pltpu.VMEM((chunks, n - 1, both // n, width // 2), BF16),
            pltpu.VMEM((chunks, both, width), BF16),
            dma((2,)), dma((2,)), dma((5,)), dma((1,)), dma((chunks, 2)),
            dma((2, 2)), dma((2, 2)), dma((1,)), dma((1,)), dma((chunks,)), dma((chunks,)), dma((chunks,)), dma((chunks,)),
            dma((chunks, n)), dma((chunks, n)), dma((chunks, n)), dma((chunks, n)),
            dma((chunks, n)), dma((chunks, n)),
        ],
        compiler_params=pltpu.CompilerParams(
            collective_id=0, has_side_effects=True, vmem_limit_bytes=63 * 1024 * 1024
        ),
        name="decode",
    )(inputs, gate, up, down, low, passing, second, first_gate, first_up)


def seconds_kernel(
    n_dp, n_tensor, rate, gate_ref, up_ref, old_ref, change_ref, out_ref, change_out_ref,
    change, summed, heard, whole, raw, block, take, ring, old, fresh,
    load_sem, old_sem, store_sem, mate_send, mate_recv, ring_send, ring_recv, across_send, across_recv,
    change_sem, hear_send, hear_recv,
):
    place = Place(n_dp)
    n = place.chips
    depth = n // 2
    rank = raw.shape[1]
    units = block.shape[2]
    kept = n // n_tensor
    cuts = ring_send.shape[2]
    cut = 2 * rank // cuts

    loads = [pltpu.make_async_copy(ref, raw.at[p], load_sem.at[p]) for p, ref in enumerate((gate_ref, up_ref))]
    for load in loads:
        load.start()
    held = pltpu.make_async_copy(old_ref, old, old_sem.at[0])
    held.start()
    change_load = pltpu.make_async_copy(change_ref, change, change_sem.at[0])
    change_load.start()
    greet((place.across, place.mate, place.after, place.before) + tuple(place.flips[1:]))
    change_load.wait()
    rounds = len(place.flips)

    lines = heard.shape[1]

    def hear(i):
        if i == 0:
            src = change.at[pl.ds(pl.multiple_of((1 - place.core) * lines, lines), lines), :]
        else:
            src = summed.at[i - 1]
        return remote(src, heard.at[i], hear_send.at[i], hear_recv.at[i], place.flips[i])

    def gather(i):
        hear(i).wait()
        mine = pl.ds(pl.multiple_of(place.core * lines, lines), lines)
        before = change[mine, :] if i == 0 else summed[i - 1]
        value = (before.astype(F32) + heard[i].astype(F32)).astype(BF16)
        if i + 1 < rounds:
            summed[i] = value
            hear(i + 1).start()
        else:
            whole[mine, :] = value

    def complete():
        mine = pl.ds(pl.multiple_of(place.core * lines, lines), lines)
        return remote(whole.at[mine, :], whole.at[mine, :], hear_send.at[rounds], hear_recv.at[rounds], place.mate)

    hear(0).start()
    for load in loads:
        load.wait()

    exchanges = []
    for j in range(kept):
        for k in (2 * j, 2 * j + 1):
            for p in range(2):
                block[k, p * rank : (p + 1) * rank, :] = raw[p, :, k * units : (k + 1) * units]
        exchange = remote(
            block.at[2 * j + 1 - place.core], take.at[j], mate_send.at[j], mate_recv.at[j], place.mate
        )
        exchange.start()
        exchanges.append(exchange)
    gather(0)
    for exchange in exchanges:
        exchange.wait()
    held.wait()

    def target(index):
        index = lax.rem(index + 2 * n, n)
        where = jnp.where(place.core == 0, index, lax.rem(n - index, n))
        y = jnp.where(where < depth, 0, 1)
        z = jnp.where(where < depth, where, n - 1 - where)
        per = depth // n_tensor
        return z // per == place.t, lax.rem(z, per) * 2 + y

    def hop(d, j, u):
        own = pl.ds(u * cut, cut)
        return remote(
            block.at[2 * j + place.core, own, :], ring.at[d, j, own, :],
            ring_send.at[d, j, u], ring_recv.at[d, j, u], (place.after, place.before)[d],
        )

    def final(u):
        own = pl.ds(u * cut, cut)
        return remote(fresh.at[own, :], fresh.at[own, :], across_send.at[u], across_recv.at[u], place.across)

    up, down = n // 2, n - 1 - n // 2
    sends = [
        (s, d, target(place.turn + (up - s if d == 0 else s - down)))
        for s in range(up) for d, count in ((0, up), (1, down)) if s < count
    ]

    def mix(j, u):
        own = pl.ds(u * cut, cut)
        return block[2 * j + place.core, own, :].astype(F32) + take[j, own, :].astype(F32)

    for s, d, (active, j) in sends:

        @pl.when(active)
        def _():
            for u in range(cuts):
                own = pl.ds(u * cut, cut)
                value = mix(j, u)
                if s > 0:
                    hop(d, j, u).wait_recv()
                    value = value + ring[d, j, own, :].astype(F32)
                block[2 * j + place.core, own, :] = value.astype(BF16)
                hop(d, j, u).start()

        if d == 0 and 1 <= s < rounds - 1:
            gather(s)

    owner, j = target(place.turn)

    @pl.when(owner)
    def _():
        for u in range(cuts):
            own = pl.ds(u * cut, cut)
            value = mix(j, u)
            for d in range(2):
                hop(d, j, u).wait_recv()
                value = value + ring[d, j, own, :].astype(F32)
            fresh[own, :] = (old[own, :].astype(F32) - rate * value).astype(BF16)
            final(u).start()

    gather(rounds - 1)
    complete().start()
    for s, d, (active, j) in sends:

        @pl.when(active)
        def _():
            for u in range(cuts):
                hop(d, j, u).wait_send()

    @pl.when(owner)
    def _():
        for u in range(cuts):
            final(u).wait_send()

    @pl.when(jnp.logical_not(owner))
    def _():
        for u in range(cuts):
            final(u).wait_recv()

    complete().wait()
    stores = [
        pltpu.make_async_copy(fresh, out_ref, store_sem.at[0]),
        pltpu.make_async_copy(whole, change_out_ref, change_sem.at[1]),
    ]
    for store in stores:
        store.start()
    for store in stores:
        store.wait()


def new_seconds(gate_gradient, up_gradient, old, change, rate):
    rounds = 4
    n_dp, n_tensor = lax.axis_size("dp"), lax.axis_size("tensor")
    both, units = old.shape
    n = n_dp // 2
    kept, cuts = n // n_tensor, 4
    dma = pltpu.SemaphoreType.DMA
    anywhere = pl.BlockSpec(memory_space=pl.ANY)
    return pl.pallas_call(
        functools.partial(seconds_kernel, n_dp, n_tensor, rate),
        out_shape=(jax.ShapeDtypeStruct((both, units), BF16), jax.ShapeDtypeStruct(change.shape, BF16)),
        in_specs=[anywhere] * 4,
        out_specs=(anywhere, anywhere),
        scratch_shapes=[
            pltpu.VMEM(change.shape, BF16),
            pltpu.VMEM((rounds - 1, change.shape[0] // 2, both), BF16),
            pltpu.VMEM((rounds, change.shape[0] // 2, both), BF16),
            pltpu.VMEM(change.shape, BF16),
            pltpu.VMEM((2, both // 2, gate_gradient.shape[1]), BF16),
            pltpu.VMEM((2 * kept, both, units), BF16),
            pltpu.VMEM((kept, both, units), BF16),
            pltpu.VMEM((2, kept, both, units), BF16),
            pltpu.VMEM((both, units), BF16),
            pltpu.VMEM((both, units), BF16),
            dma((2,)), dma((1,)), dma((1,)),
            dma((kept,)), dma((kept,)), dma((2, kept, cuts)), dma((2, kept, cuts)), dma((cuts,)), dma((cuts,)),
            dma((2,)), dma((rounds + 1,)), dma((rounds + 1,)),
        ],
        compiler_params=pltpu.CompilerParams(
            collective_id=1, has_side_effects=True, vmem_limit_bytes=28 * 1024 * 1024
        ),
        cost_estimate=pl.CostEstimate(flops=0, bytes_accessed=100_000_000, transcendentals=0),
        name="seconds",
    )(gate_gradient, up_gradient, old, change)


def on_device(
    training_token_input,
    gate_output_gradient,
    up_output_gradient,
    gate_first_matrix,
    gate_second_matrix,
    up_first_matrix,
    up_second_matrix,
    gate_weight_base,
    up_weight_base,
    down_weight_base,
    decode_step_input,
):
    f32, bf16 = jnp.float32, jnp.bfloat16
    n_dp, n_tensor = lax.axis_size("dp"), lax.axis_size("tensor")
    me = lax.axis_index("tensor")
    replica = lax.axis_index("dp")
    rank = gate_first_matrix.shape[1]
    tokens_total = training_token_input.shape[0] * n_dp
    second_learning_rate = 0.5 / math.sqrt(ADAPTER_RANK * tokens_total)
    first_learning_rate = 0.5 / math.sqrt(MODEL_WIDTH * HIDDEN_UNITS * tokens_total / ADAPTER_RANK)
    kernels = n_tensor == 2 and n_dp == 16 and decode_step_input.shape[0] == 2

    def dot(left, right, over):
        return lax.dot_general(left, right, (over, ((), ())), preferred_element_type=f32)

    firsts = jnp.concatenate([gate_first_matrix, up_first_matrix], axis=1)
    inner = jnp.concatenate(
        [
            jnp.dot(training_token_input, firsts, preferred_element_type=f32),
            dot(gate_output_gradient, gate_second_matrix, ((1,), (1,))),
            dot(up_output_gradient, up_second_matrix, ((1,), (1,))),
        ],
        axis=1,
    )
    inner, rows_in = lax.optimization_barrier((inner.astype(bf16), decode_step_input))
    inner = pair_sum(inner).astype(bf16)
    inner_b, inner_a = inner[:, : 2 * rank], inner[:, 2 * rank :]

    columns = gate_weight_base.shape[1]
    group = n_dp // n_tensor
    steps = rows_in.shape[0]
    if kernels:
        theirs = row_share(rows_in, 1 - me)[0]
        arrived = [
            swap(jnp.dot(theirs, weight, preferred_element_type=f32).astype(bf16))
            for weight in (gate_weight_base, up_weight_base)
        ]
        similar = dot(rows_in, training_token_input, ((2,), (1,))).astype(bf16)
        change = dot(similar, inner_a, ((2,), (0,))).astype(bf16)
        block = lax.rem(replica, group)

        def old_block(matrix):
            return lax.dynamic_slice_in_dim(matrix, block * columns, columns, 1)

        seconds, change = new_seconds(
            dot(inner_b[:, :rank], gate_output_gradient, ((0,), (0,))).astype(bf16),
            dot(inner_b[:, rank:], up_output_gradient, ((0,), (0,))).astype(bf16),
            jnp.concatenate([old_block(gate_second_matrix), old_block(up_second_matrix)], axis=0),
            change.reshape(-1, 2 * rank),
            second_learning_rate,
        )
        low = dot(rows_in, firsts, ((2,), (0,))) - first_learning_rate * change.reshape(
            steps, -1, 2 * rank
        ).astype(f32)
    else:
        unit = 16 * n_tensor
        padded = -(-columns // unit) * unit
        piece = padded // n_tensor
        second_gradient = jnp.concatenate(
            [
                dot(gate_output_gradient, inner_b[:, :rank], ((0,), (0,))).astype(bf16),
                dot(up_output_gradient, inner_b[:, rank:], ((0,), (0,))).astype(bf16),
            ],
            axis=1,
        )
        second_gradient = jnp.pad(
            second_gradient.reshape(group, columns, 2 * rank),
            ((0, 0), (0, padded - columns), (0, 0)),
        ).reshape(group * padded, 2 * rank)
        first_gradient = dot(training_token_input, inner_a, ((0,), (0,))).astype(bf16)
        rows_in, second_gradient, first_gradient = lax.optimization_barrier(
            (rows_in, second_gradient, first_gradient)
        )
        second_gradient = lax.psum_scatter(second_gradient, "dp", scatter_dimension=0, tiled=True)
        first_gradient = lax.psum(first_gradient, "dp")
        start = replica // n_tensor * columns + replica % n_tensor * piece

        def old_piece(matrix):
            wide = jnp.pad(matrix, ((0, 0), (0, padded)))
            return lax.dynamic_slice_in_dim(wide, start, piece, 1).T

        old = jnp.concatenate([old_piece(gate_second_matrix), old_piece(up_second_matrix)], axis=1)
        stepped = (
            old.astype(f32) - second_learning_rate * second_gradient.astype(f32)
        ).astype(bf16)
        routes = [
            (
                (block * n_tensor + part) * n_tensor + side,
                (side * group + block) * n_tensor + part,
            )
            for block in range(group)
            for part in range(n_tensor)
            for side in range(n_tensor)
        ]
        stepped = lax.ppermute(stepped, ("dp", "tensor"), routes)
        seconds = lax.all_gather(stepped, "tensor", axis=0, tiled=True)[:columns].T
        new_firsts = (
            firsts.astype(f32) - first_learning_rate * first_gradient.astype(f32)
        ).astype(bf16)
        low = dot(rows_in, new_firsts, ((2,), (0,)))
        low = lax.psum_scatter(
            low.astype(bf16), "tensor", scatter_dimension=1, tiled=True
        ).astype(bf16)

    def base(rows, weight):
        return dot(rows, weight, ((2,), (0,))).astype(bf16)

    weights = (gate_weight_base, up_weight_base)
    if kernels:

        def share_of(side):
            value = row_share(low, side).astype(bf16).reshape(-1, 2 * rank)
            return jnp.stack([value[:, :rank], value[:, rank:]])

        result = decode(
            rows_in.reshape(-1, rows_in.shape[2]),
            gate_weight_base.T,
            up_weight_base.T,
            down_weight_base,
            share_of(me),
            share_of(1 - me),
            seconds.reshape(2, rank, columns),
            *arrived,
            steps,
        )
        return result.reshape(steps, -1, result.shape[1])

    base_sums = [
        lax.psum_scatter(
            base(rows_in, weight), "tensor", scatter_dimension=1, tiled=True
        ).astype(f32)
        for weight in weights
    ]
    gate = base_sums[0] + dot(low[..., :rank], seconds[:rank], ((2,), (0,)))
    upper = base_sums[1] + dot(low[..., rank:], seconds[rank:], ((2,), (0,)))
    hidden = (jax.nn.silu(gate) * upper).astype(bf16)

    hidden = lax.all_gather(hidden, "tensor", axis=1, tiled=True)
    steps, rows, _ = hidden.shape
    out = dot(hidden, down_weight_base, ((2,), (0,))).astype(bf16)
    out = out.reshape(steps * rows, -1)
    out = lax.psum_scatter(out, "dp", scatter_dimension=0, tiled=True)
    out = lax.all_gather(out, "dp", axis=0, tiled=True)
    return out.reshape(steps, rows, -1)


def solution(mesh):
    placed = (
        P("dp", "tensor"),
        P("dp", "tensor"),
        P("dp", "tensor"),
        P("tensor", None),
        P(None, "tensor"),
        P("tensor", None),
        P(None, "tensor"),
        P("tensor", "dp"),
        P("tensor", "dp"),
        P("dp", "tensor"),
        P(None, None, "tensor"),
    )
    return jax.shard_map(
        on_device, mesh=mesh, in_specs=placed, out_specs=P(None, None, "tensor"), check_vma=False
    )
```
